32 devices in a mesh: vocab: 8 (over z, x), dp: 4 (over y, core).
Axes of the slice: x: 2, y: 2, z: 4, core: 2. Of those that a mesh axis runs over, the one named last changes fastest.
Arguments:
- out_grads: float32 [4096, 4096], P(('vocab', 'dp')), may hold values from -6 to 6
- token_ids: int32 [4096], P(('vocab', 'dp')), may hold values from 0 to 128255, as said below
Outputs:
- table_grad: bfloat16 [128256, 4096], P('vocab', 'dp')
The draws below stay inside these ranges and needn't reach their ends.
Inputs may be any that keep to these rules, and one draw needn't show every extreme that they name: `token_ids`: call ids k * 16032 to (k + 1) * 16032 - 1 block k. The 128 tokens of one device hold at most 48 ids of any one block; one block, the same for all devices, holds exactly 48 ids of every device.
All inputs are finite; a program needn't handle non-finite values.
Results may differ from the reference program's by a relative error of at most 0.001.
Values sent between devices are 32-bit elements; how exact they have to be, the bound alone decides.
A program may use at most 192 MiB of HBM per device.

```python
import jax
import jax.numpy as jnp
from jax import lax

D = 4096
VOCAB = 128256
TOK_DEV = 128
TOKENS = 4096
N_VOCAB = 8
N_DP = 4


def draw_token_ids(key, part):
    rows_own = VOCAB // N_VOCAB
    capacity = 3 * TOK_DEV // N_VOCAB
    key_hot, key_rest = jax.random.split(jax.random.fold_in(key, 71))
    hot_block = jax.random.randint(key_hot, (), 0, N_VOCAB).astype(jnp.int32)

    def one_device(sub_key):
        key_pick, key_order, key_first, key_second = jax.random.split(sub_key, 4)
        others = (hot_block + 1 + jnp.arange((N_VOCAB - 1) * capacity, dtype=jnp.int32) // capacity) % N_VOCAB
        picked = jax.random.permutation(key_pick, others)[:TOK_DEV - capacity]
        owners = jnp.concatenate([jnp.full((capacity,), hot_block, jnp.int32), picked.astype(jnp.int32)])
        owners = jax.random.permutation(key_order, owners)
        first = jax.random.randint(key_first, (TOK_DEV,), 0, rows_own).astype(jnp.int32)
        second = jax.random.randint(key_second, (TOK_DEV,), 0, rows_own).astype(jnp.int32)
        inside = first * second // rows_own
        return (owners * rows_own + inside).astype(jnp.int32)
    device_keys = jax.random.split(key_rest, N_VOCAB * N_DP)
    return jax.vmap(one_device)(device_keys).reshape(-1).astype(jnp.int32)


def level_of(rng, shape, cuts, low, top_value):
    loudness = 1.0
    for axis_at, shards_of in cuts:
        heights = jax.random.uniform(jax.random.fold_in(jax.random.fold_in(rng, 6), axis_at), (shards_of,), jnp.float32, low / len(cuts), top_value / len(cuts))
        loudness = loudness * jnp.repeat(jnp.exp(heights), shape[axis_at] // shards_of).reshape((-1,) + (1,) * (len(shape) - 1 - axis_at))
    return loudness


def centred(rng, shape, spread, most, shards=(), kind=jnp.bfloat16):
    factor_of = level_of(rng, shape, shards, -0.22, 0.18) if shards else 1.0
    result = jax.random.normal(rng, shape, jnp.float32) * spread * factor_of
    return jnp.minimum(jnp.maximum(result, -most), most).astype(kind)


def setup_inputs(seed: int = 0) -> dict:
    streams_of = jax.random.split(jax.random.key(seed), 3)
    out_grads = centred(streams_of[0], (TOKENS, D), 1.0, 6.0, ((0, 32),), jnp.float32)
    token_ids = draw_token_ids(jax.random.fold_in(streams_of[2], 71), 0)
    return dict(out_grads=out_grads, token_ids=token_ids)


def reference(out_grads, token_ids):
    width_block = 256 if D % 256 == 0 else D
    blocks = D // width_block
    pieces = out_grads.reshape(TOKENS, blocks, width_block).transpose(1, 0, 2)

    def one_block(piece):
        summed = jax.ops.segment_sum(piece, token_ids, num_segments=VOCAB)
        return summed.astype(jnp.bfloat16)

    table = lax.map(one_block, pieces)
    return table.transpose(1, 0, 2).reshape(VOCAB, D)
```

```python
import functools
import math

import jax
import jax.numpy as jnp
from jax import lax
from jax.experimental import pallas as pl
from jax.experimental.pallas import tpu as pltpu
from jax.sharding import PartitionSpec as P

VOCAB = 128256
LANES = 128


def ranks_in_block(owner_of):
    positions = lax.iota(jnp.int32, owner_of.shape[1])
    earlier = (owner_of[:, :, None] == owner_of[:, None, :]) & (positions[None, None, :] < positions[None, :, None])
    return jnp.sum(earlier.astype(jnp.int32), axis=2)


def pack_kernel(dp, chunks, picks_ref, data_ref, out_ref):
    slots = out_ref.shape[1]

    @pl.loop(0, slots)
    def _(slot):
        token = picks_ref[slot]
        base = token // 8 * (8 * chunks * dp) + token % 8
        for column in range(dp):
            out_ref[column, slot] = data_ref[pl.ds(base + column * (8 * chunks), chunks, stride=8), :]


def pack(out_grads, picks, dp):
    tok_count, width = out_grads.shape
    chunks = width // dp // LANES
    data = out_grads.reshape(tok_count // 8, 8, width // LANES, LANES).transpose(0, 2, 1, 3).reshape(-1, LANES)
    return pl.pallas_call(
        functools.partial(pack_kernel, dp, chunks),
        out_shape=jax.ShapeDtypeStruct((dp, picks.shape[0], chunks, LANES), out_grads.dtype),
        in_specs=[pl.BlockSpec(memory_space=pltpu.SMEM), pl.BlockSpec(memory_space=pltpu.VMEM)],
        out_specs=pl.BlockSpec(memory_space=pltpu.VMEM),
        compiler_params=pltpu.CompilerParams(vmem_limit_bytes=24 * 2**20),
        name="pack",
    )(picks, data)


def gather_kernel(n, dp, ids_ref, ids_all, ids_out, ids_in, own_sem):
    v, d = lax.axis_index("vocab"), lax.axis_index("dp")
    me = v * dp + d
    others = n * dp - 1
    own = pltpu.make_async_copy(ids_ref, ids_all.at[me], own_sem)
    own.start()

    def send(i, _):
        k = others - i
        where = dict(device_id=(flip(v, k // dp, n), (d + k % dp) % dp), device_id_type=pl.DeviceIdType.MESH)
        pltpu.make_async_remote_copy(ids_ref, ids_all.at[me], ids_out, ids_in, **where).start()
        return 0

    lax.fori_loop(0, others, send, 0)
    own.wait()
    all_ids = ids_all.at[pl.ds(0, others)]
    for sem in (ids_out, ids_in):
        pltpu.make_async_copy(all_ids, all_ids, sem).wait()


def gather_ids(ids, n, dp):
    return pl.pallas_call(
        functools.partial(gather_kernel, n, dp),
        out_shape=jax.ShapeDtypeStruct((n * dp,) + ids.shape, ids.dtype),
        in_specs=[pl.BlockSpec(memory_space=pl.ANY)],
        out_specs=pl.BlockSpec(memory_space=pl.ANY),
        scratch_shapes=[pltpu.SemaphoreType.DMA] * 3,
        compiler_params=pltpu.CompilerParams(has_side_effects=True),
        name="gather_ids",
    )(ids)


def flip(a, k, n):
    total, bit = 0, 1
    while bit < n:
        total = total + (((a // bit) % 2) + ((k // bit) % 2)) % 2 * bit
        bit *= 2
    return total


def exchange_kernel(n, dp, hot, most, few, picked_ref, arrived, sem_out, sem_in, own_sem):
    v, d = lax.axis_index("vocab"), lax.axis_index("dp")
    me = v * dp + d
    others = n * dp - 1

    def rows_of(block, column, count):
        source = picked_ref.at[column, pl.ds(block * most, count)]
        return source, arrived.at[pl.ds(me * most, count)]

    def send(i, _):
        k = i + 1
        block, column = flip(v, k // dp, n), (d + k % dp) % dp
        where = dict(device_id=(block, column), device_id_type=pl.DeviceIdType.MESH)

        @pl.when(block == hot)
        def _():
            pltpu.make_async_remote_copy(*rows_of(block, column, most), sem_out, sem_in, **where).start()

        @pl.when(block != hot)
        def _():
            pltpu.make_async_remote_copy(*rows_of(block, column, few), sem_out, sem_in, **where).start()

        return 0

    lax.fori_loop(0, others, send, 0)
    own = pltpu.make_async_copy(*rows_of(v, d, most), own_sem)
    own.start()
    own.wait()

    def drain(sem, count):
        rows = arrived.at[pl.ds(0, count)]
        pltpu.make_async_copy(rows, rows, sem).wait()

    @pl.when(v == hot)
    def _():
        drain(sem_out, (dp - 1) * most + (n - 1) * dp * few)
        drain(sem_in, others * most)

    @pl.when(v != hot)
    def _():
        drain(sem_out, dp * most + ((n - 1) * dp - 1) * few)
        drain(sem_in, others * few)


def exchange(n, dp, most, hot, few, picked):
    name = "exchange_all" if few == most else f"exchange_{hot}_{few}"
    return pl.pallas_call(
        functools.partial(exchange_kernel, n, dp, hot, most, few),
        out_shape=jax.ShapeDtypeStruct((n * dp * most,) + picked.shape[2:], picked.dtype),
        in_specs=[pl.BlockSpec(memory_space=pltpu.VMEM)],
        out_specs=pl.BlockSpec(memory_space=pl.ANY),
        scratch_shapes=[pltpu.SemaphoreType.DMA] * 3,
        compiler_params=pltpu.CompilerParams(has_side_effects=True, vmem_limit_bytes=24 * 2**20),
        name=name,
    )(picked)


def order_slots(ids_all, block, rows_own, capacity, tile):
    devices = ids_all.shape[0]
    mine = (ids_all // rows_own) == block
    positions = lax.iota(jnp.int32, ids_all.shape[1])
    before = mine[:, None, :] & (positions[None, None, :] < positions[None, :, None])
    rank = jnp.sum(before.astype(jnp.int32), axis=2)
    slot_ids = lax.iota(jnp.int32, capacity)
    hit = mine[:, None, :] & (rank[:, None, :] == slot_ids[None, :, None])
    local_row = ids_all - block * rows_own
    row_at = jnp.sum(jnp.where(hit, local_row[:, None, :] + 1, 0), axis=2) - 1
    row_at = row_at.reshape(-1)
    total = devices * capacity
    slots = lax.iota(jnp.int32, total)
    key = jnp.where(row_at >= 0, row_at, rows_own) * total + slots
    place = jnp.sum((key[None, :] < key[:, None]).astype(jnp.int32), axis=1)
    sorted_key = jnp.sum(jnp.where(place[None, :] == slots[:, None], key[None, :], 0), axis=1)
    sorted_row = sorted_key // total
    sorted_slot = sorted_key - sorted_row * total
    tiles = pl.cdiv(rows_own, tile)
    bounds = jnp.minimum(lax.iota(jnp.int32, tiles + 1) * tile, rows_own)
    row_key = key // total
    starts = jnp.sum((row_key[None, :] < bounds[:, None]).astype(jnp.int32), axis=1)
    return sorted_slot, sorted_row, starts


def table_kernel(tile, chunks, slots_ref, rows_ref, starts_ref, data_ref, out_ref, acc):
    step = pl.program_id(0)
    base = step * tile

    @pl.when(step == 0)
    def _():
        acc[...] = jnp.zeros_like(acc)

    def place(at):
        row = rows_ref[at] - base
        return pl.ds(row // 8 * (8 * chunks) + row % 8, chunks, stride=8)

    @pl.loop(starts_ref[step], starts_ref[step + 1])
    def _(at):
        acc[place(at), :] += data_ref[slots_ref[at]]

    @pl.loop(0, tile // 16)
    def _(group):
        low = group * (16 * chunks)
        high = low + 8 * chunks
        for chunk in range(chunks):
            pair = [acc[pl.ds(pl.multiple_of(half + chunk * 8, 8), 8), :] for half in (low, high)]
            out_ref[pl.ds(pl.multiple_of(group * 16, 16), 16), chunk * LANES : (chunk + 1) * LANES] = jnp.concatenate(
                pair, axis=0
            ).astype(out_ref.dtype)

    @pl.loop(starts_ref[step], starts_ref[step + 1])
    def _(at):
        acc[place(at), :] = jnp.zeros((chunks, LANES), acc.dtype)


def build_table(data, slots, rows, starts, rows_own, tile):
    count, chunks, _ = data.shape
    width = chunks * LANES
    tiles = pl.cdiv(rows_own, tile)
    return pl.pallas_call(
        functools.partial(table_kernel, tile, chunks),
        out_shape=jax.ShapeDtypeStruct((rows_own, width), jnp.bfloat16),
        grid_spec=pltpu.PrefetchScalarGridSpec(
            num_scalar_prefetch=3,
            grid=(tiles,),
            in_specs=[
                pl.BlockSpec((count, chunks, LANES), lambda i, *_: (0, 0, 0), pipeline_mode=pl.Buffered(1))
            ],
            out_specs=pl.BlockSpec((tile, width), lambda i, *_: (i, 0)),
            scratch_shapes=[pltpu.VMEM((tile * chunks, LANES), jnp.float32)],
        ),
        compiler_params=pltpu.CompilerParams(vmem_limit_bytes=40 * 2**20),
        name="table",
    )(slots, rows, starts, data)


def local(out_grads, token_ids):
    owners, dp = lax.axis_size("vocab"), lax.axis_size("dp")
    tok_count, width = out_grads.shape
    rows_own = VOCAB // owners
    most = 3 * tok_count // owners
    tile = 1024
    mean = (tok_count - most) / (owners - 1)
    levels = [min(most, math.ceil(mean + spread * math.sqrt(mean))) for spread in (2.3, 3.6)]

    owner_of = token_ids // rows_own
    rank = ranks_in_block(owner_of[None])[0]
    target = owner_of * most + rank
    tokens = lax.iota(jnp.int32, tok_count)
    hit = target[None, :] == lax.iota(jnp.int32, owners * most)[:, None]
    picks = jnp.sum(jnp.where(hit, tokens[None, :], 0), axis=1)
    picked = pack(out_grads, picks, dp)

    ids_all = gather_ids(token_ids[None], owners, dp)[:, 0]
    blocks = lax.iota(jnp.int32, owners)
    counts = jnp.sum((ids_all[None] // rows_own == blocks[:, None, None]).astype(jnp.int32), axis=2)
    full = jnp.min(counts, axis=1) == most
    hot = jnp.min(jnp.where(full, blocks, owners))
    cold_most = jnp.max(jnp.where(blocks[:, None] == hot, 0, counts))
    branch = owners * len(levels)
    for at in reversed(range(len(levels))):
        branch = jnp.where((cold_most <= levels[at]) & (hot < owners), owners * at + hot, branch)
    slots, rows, starts = order_slots(ids_all, lax.axis_index("vocab"), rows_own, most, tile)

    sends = [functools.partial(exchange, owners, dp, most, block, few) for few in levels for block in range(owners)]
    sends.append(functools.partial(exchange, owners, dp, most, 0, most))
    data = lax.switch(branch, sends, picked)
    return build_table(data, slots, rows, starts, rows_own, tile)


def solution(mesh):
    in_specs = (P(("vocab", "dp"), None), P(("vocab", "dp")))
    out_specs = P("vocab", "dp")
    return jax.shard_map(local, mesh=mesh, in_specs=in_specs, out_specs=out_specs, check_vma=False)
```

```python
import functools
import math

import jax
import jax.numpy as jnp
from jax import lax
from jax.experimental import pallas as pl
from jax.experimental.pallas import tpu as pltpu
from jax.sharding import PartitionSpec as P

VOCAB = 128256
LANES = 128


def ranks_in_block(owner_of):
    positions = lax.iota(jnp.int32, owner_of.shape[1])
    earlier = (owner_of[:, :, None] == owner_of[:, None, :]) & (positions[None, None, :] < positions[None, :, None])
    return jnp.sum(earlier.astype(jnp.int32), axis=2)


def pack_kernel(dp, chunks, picks_ref, data_ref, out_ref):
    slots = out_ref.shape[1]

    @pl.loop(0, slots, unroll=8)
    def _(slot):
        base = picks_ref[slot]
        for column in range(dp):
            out_ref[column, slot] = data_ref[pl.ds(base + column * (8 * chunks), chunks, stride=8), :]


def pack(out_grads, picks, dp):
    tok_count, width = out_grads.shape
    chunks = width // dp // LANES
    data = out_grads.reshape(tok_count // 8, 8, width // LANES, LANES).transpose(0, 2, 1, 3).reshape(-1, LANES)
    return pl.pallas_call(
        functools.partial(pack_kernel, dp, chunks),
        out_shape=jax.ShapeDtypeStruct((dp, picks.shape[0], chunks, LANES), out_grads.dtype),
        in_specs=[pl.BlockSpec(memory_space=pltpu.SMEM), pl.BlockSpec(memory_space=pltpu.VMEM)],
        out_specs=pl.BlockSpec(memory_space=pltpu.VMEM),
        compiler_params=pltpu.CompilerParams(vmem_limit_bytes=24 * 2**20),
        name="pack",
    )(picks, data)


def gather_kernel(n, dp, ids_ref, ids_all, ids_out, ids_in, own_sem):
    v, d = lax.axis_index("vocab"), lax.axis_index("dp")
    me = v * dp + d
    others = n * dp - 1
    own = pltpu.make_async_copy(ids_ref, ids_all.at[me], own_sem)
    own.start()

    def send(i, _):
        k = others - i
        where = dict(device_id=(flip(v, k // dp, n), (d + k % dp) % dp), device_id_type=pl.DeviceIdType.MESH)
        pltpu.make_async_remote_copy(ids_ref, ids_all.at[me], ids_out, ids_in, **where).start()
        return 0

    lax.fori_loop(0, others, send, 0)
    own.wait()
    all_ids = ids_all.at[pl.ds(0, others)]
    for sem in (ids_out, ids_in):
        pltpu.make_async_copy(all_ids, all_ids, sem).wait()


def gather_ids(ids, n, dp):
    return pl.pallas_call(
        functools.partial(gather_kernel, n, dp),
        out_shape=jax.ShapeDtypeStruct((n * dp,) + ids.shape, ids.dtype),
        in_specs=[pl.BlockSpec(memory_space=pltpu.VMEM)],
        out_specs=pl.BlockSpec(memory_space=pltpu.VMEM),
        scratch_shapes=[pltpu.SemaphoreType.DMA] * 3,
        compiler_params=pltpu.CompilerParams(has_side_effects=True),
        name="gather_ids",
    )(ids)


def flip(a, k, n):
    total, bit = 0, 1
    while bit < n:
        total = total + (((a // bit) % 2) + ((k // bit) % 2)) % 2 * bit
        bit *= 2
    return total


def exchange_kernel(n, dp, hot, most, few, picked_ref, arrived, sem_out, sem_in, own_sem):
    v, d = lax.axis_index("vocab"), lax.axis_index("dp")
    me = v * dp + d
    others = n * dp - 1

    def rows_of(block, column, count):
        source = picked_ref.at[column, pl.ds(block * most, count)]
        return source, arrived.at[pl.ds(me * most, count)]

    def send(i, _):
        k = i + 1
        block, column = flip(v, k // dp, n), (d + k % dp) % dp
        where = dict(device_id=(block, column), device_id_type=pl.DeviceIdType.MESH)

        @pl.when(block == hot)
        def _():
            pltpu.make_async_remote_copy(*rows_of(block, column, most), sem_out, sem_in, **where).start()

        @pl.when(block != hot)
        def _():
            pltpu.make_async_remote_copy(*rows_of(block, column, few), sem_out, sem_in, **where).start()

        return 0

    lax.fori_loop(0, others, send, 0)
    own = pltpu.make_async_copy(*rows_of(v, d, most), own_sem)
    own.start()
    own.wait()

    def drain(sem, count):
        rows = arrived.at[pl.ds(0, count)]
        pltpu.make_async_copy(rows, rows, sem).wait()

    @pl.when(v == hot)
    def _():
        drain(sem_out, (dp - 1) * most + (n - 1) * dp * few)
        drain(sem_in, others * most)

    @pl.when(v != hot)
    def _():
        drain(sem_out, dp * most + ((n - 1) * dp - 1) * few)
        drain(sem_in, others * few)


def exchange(n, dp, most, hot, few, picked):
    name = "exchange_all" if few == most else f"exchange_{hot}_{few}"
    return pl.pallas_call(
        functools.partial(exchange_kernel, n, dp, hot, most, few),
        out_shape=jax.ShapeDtypeStruct((n * dp * most,) + picked.shape[2:], picked.dtype),
        in_specs=[pl.BlockSpec(memory_space=pltpu.VMEM)],
        out_specs=pl.BlockSpec(memory_space=pl.ANY),
        scratch_shapes=[pltpu.SemaphoreType.DMA] * 3,
        compiler_params=pltpu.CompilerParams(has_side_effects=True, vmem_limit_bytes=24 * 2**20),
        name=name,
    )(picked)


def order_slots(ids_all, block, rows_own, capacity, tile):
    devices = ids_all.shape[0]
    mine = (ids_all // rows_own) == block
    positions = lax.iota(jnp.int32, ids_all.shape[1])
    before = mine[:, None, :] & (positions[None, None, :] < positions[None, :, None])
    rank = jnp.sum(before.astype(jnp.int32), axis=2)
    slot_ids = lax.iota(jnp.int32, capacity)
    hit = mine[:, None, :] & (rank[:, None, :] == slot_ids[None, :, None])
    local_row = ids_all - block * rows_own
    row_at = jnp.sum(jnp.where(hit, local_row[:, None, :] + 1, 0), axis=2) - 1
    row_at = row_at.reshape(-1)
    total = devices * capacity
    slots = lax.iota(jnp.int32, total)
    key = jnp.where(row_at >= 0, row_at, rows_own) * total + slots
    place = jnp.sum((key[None, :] < key[:, None]).astype(jnp.int32), axis=1)
    sorted_key = jnp.sum(jnp.where(place[None, :] == slots[:, None], key[None, :], 0), axis=1)
    sorted_row = sorted_key // total
    sorted_slot = sorted_key - sorted_row * total
    tiles = pl.cdiv(rows_own, tile)
    bounds = jnp.minimum(lax.iota(jnp.int32, tiles + 1) * tile, rows_own)
    row_key = key // total
    starts = jnp.sum((row_key[None, :] < bounds[:, None]).astype(jnp.int32), axis=1)
    return sorted_slot, sorted_row, starts


def table_kernel(tile, batch, slots_ref, rows_ref, starts_ref, data_ref, out_ref, data, acc, held, last_held, sems, data_sem):
    rows_own, width = out_ref.shape
    buffers = held.shape[0]
    full = rows_own // tile
    fetch = pltpu.make_async_copy(data_ref, data, data_sem)
    fetch.start()
    acc[...] = jnp.zeros_like(acc)
    fetch.wait()

    def fill(step, target):
        base = step * tile
        start, end = starts_ref[step], starts_ref[step + 1]
        batches = (end - start + batch - 1) // batch

        def row_at(at):
            return jnp.where(at < end, rows_ref[at] - base, tile)

        def add(index, carry):
            total, last = carry
            for at in range(batch):
                at += start + index * batch
                row = row_at(at)
                total = jnp.where(row == last, total, 0.0) + data[slots_ref[at]]
                acc[pl.ds(row, 1), :] = total.reshape(1, width)
                last = row
            return total, last

        lax.fori_loop(0, batches, add, (jnp.zeros(data.shape[1:], acc.dtype), jnp.int32(-1)))
        target[...] = acc[: target.shape[0], :].astype(target.dtype)

        @pl.loop(0, batches)
        def _(index):
            for at in range(batch):
                acc[pl.ds(row_at(at + start + index * batch), 1), :] = jnp.zeros((1, width), acc.dtype)

    def put(step, slot):
        place = out_ref.at[pl.ds(pl.multiple_of(step * tile, tile), tile)]
        return pltpu.make_async_copy(held.at[slot], place, sems.at[slot])

    @pl.loop(0, full)
    def _(step):
        slot = step % buffers

        @pl.when(step >= buffers)
        def _():
            put(step - buffers, slot).wait()

        fill(step, held.at[slot])
        put(step, slot).start()

    if rows_own % tile:
        fill(full, last_held)
        rest = pltpu.make_async_copy(last_held, out_ref.at[pl.ds(full * tile, rows_own % tile)], data_sem)
        rest.start()
        rest.wait()
    for step in range(max(full - buffers, 0), full):
        put(step, step % buffers).wait()


def build_table(data, slots, rows, starts, rows_own, tile, buffers, batch):
    _, chunks, _ = data.shape
    width = chunks * LANES
    slots, rows = (jnp.pad(part, (0, batch)) for part in (slots, rows))
    return pl.pallas_call(
        functools.partial(table_kernel, tile, batch),
        out_shape=jax.ShapeDtypeStruct((rows_own, width), jnp.bfloat16),
        in_specs=[pl.BlockSpec(memory_space=pltpu.SMEM)] * 3 + [pl.BlockSpec(memory_space=pl.ANY)],
        out_specs=pl.BlockSpec(memory_space=pl.ANY),
        scratch_shapes=[
            pltpu.VMEM(data.shape, data.dtype),
            pltpu.VMEM((tile + 8, width), jnp.float32),
            pltpu.VMEM((buffers, tile, width), jnp.bfloat16),
            pltpu.VMEM((rows_own % tile or 16, width), jnp.bfloat16),
            pltpu.SemaphoreType.DMA((buffers,)),
            pltpu.SemaphoreType.DMA,
        ],
        compiler_params=pltpu.CompilerParams(vmem_limit_bytes=40 * 2**20),
        name="table",
    )(slots, rows, starts, data)


def local(out_grads, token_ids):
    owners, dp = lax.axis_size("vocab"), lax.axis_size("dp")
    tok_count, width = out_grads.shape
    rows_own = VOCAB // owners
    most = 3 * tok_count // owners
    tile = 512
    mean = (tok_count - most) / (owners - 1)
    levels = [min(most, math.ceil(mean + spread * math.sqrt(mean))) for spread in (2.3, 3.6)]

    owner_of = token_ids // rows_own
    rank = ranks_in_block(owner_of[None])[0]
    target = owner_of * most + rank
    tokens = lax.iota(jnp.int32, tok_count)
    first_lanes = tokens // 8 * (8 * width // LANES) + tokens % 8
    hit = target[None, :] == lax.iota(jnp.int32, owners * most)[:, None]
    picks = jnp.sum(jnp.where(hit, first_lanes[None, :], 0), axis=1)
    picked = pack(out_grads, picks, dp)

    ids_all = gather_ids(token_ids[None], owners, dp)[:, 0]
    blocks = lax.iota(jnp.int32, owners)
    counts = jnp.sum((ids_all[None] // rows_own == blocks[:, None, None]).astype(jnp.int32), axis=2)
    full = jnp.min(counts, axis=1) == most
    hot = jnp.min(jnp.where(full, blocks, owners))
    cold_most = jnp.max(jnp.where(blocks[:, None] == hot, 0, counts))
    branch = owners * len(levels)
    for at in reversed(range(len(levels))):
        branch = jnp.where((cold_most <= levels[at]) & (hot < owners), owners * at + hot, branch)
    slots, rows, starts = order_slots(ids_all, lax.axis_index("vocab"), rows_own, most, tile)

    sends = [functools.partial(exchange, owners, dp, most, block, few) for few in levels for block in range(owners)]
    sends.append(functools.partial(exchange, owners, dp, most, 0, most))
    data = lax.switch(branch, sends, picked)
    return build_table(data, slots, rows, starts, rows_own, tile, 8, 8)


def solution(mesh):
    in_specs = (P(("vocab", "dp"), None), P(("vocab", "dp")))
    out_specs = P("vocab", "dp")
    return jax.shard_map(local, mesh=mesh, in_specs=in_specs, out_specs=out_specs, check_vma=False)
```

```python
import functools
import math

import jax
import jax.numpy as jnp
from jax import lax
from jax.experimental import pallas as pl
from jax.experimental.pallas import tpu as pltpu
from jax.sharding import PartitionSpec as P

VOCAB = 128256
LANES = 128


def ranks_in_block(owner_of):
    positions = lax.iota(jnp.int32, owner_of.shape[1])
    earlier = (owner_of[:, :, None] == owner_of[:, None, :]) & (positions[None, None, :] < positions[None, :, None])
    return jnp.sum(earlier.astype(jnp.int32), axis=2)


def gather_kernel(
    n, dp, most, levels, rows_own, ids_ref, picks_ref, data_ref, ids_all, picked, branch, data, rows, ids_out, ids_in, own_sem
):
    v, d = lax.axis_index("vocab"), lax.axis_index("dp")
    me = v * dp + d
    others = n * dp - 1
    chunks = rows.shape[1]
    fetch = pltpu.make_async_copy(data_ref, data, own_sem.at[0])
    fetch.start()
    own = pltpu.make_async_copy(ids_ref, ids_all.at[me], own_sem.at[1])
    own.start()

    def send(i, _):
        k = others - i
        where = dict(device_id=(flip(v, k // dp, n), (d + k % dp) % dp), device_id_type=pl.DeviceIdType.MESH)
        pltpu.make_async_remote_copy(ids_ref, ids_all.at[me], ids_out, ids_in, **where).start()
        return 0

    lax.fori_loop(0, others, send, 0)
    fetch.wait()

    @pl.loop(0, rows.shape[0] // (8 * dp))
    def _(group):
        for token in range(8):
            for column in range(dp):
                first = group * (8 * chunks * dp) + column * (8 * chunks) + token
                rows[group * (8 * dp) + token * dp + column] = data[pl.ds(first, chunks, stride=8), :]

    @pl.loop(0, picks_ref.shape[0] // 8)
    def _(group):
        for at in range(8):
            slot = group * 8 + at
            token = picks_ref[slot]
            for column in range(dp):
                picked[column, slot] = rows[token * dp + column]

    own.wait()
    all_ids = ids_all.at[pl.ds(0, others)]
    for sem in (ids_out, ids_in):
        pltpu.make_async_copy(all_ids, all_ids, sem).wait()

    ids = ids_all[:, 0, :]
    lanes = lax.broadcasted_iota(jnp.int32, (ids.shape[0], LANES), 1)
    counts = jnp.zeros((ids.shape[0], LANES), jnp.float32)
    for block in range(n):
        inside = (ids >= block * rows_own) & (ids < (block + 1) * rows_own)
        count = jnp.sum(jnp.where(inside, 1.0, 0.0), axis=1, keepdims=True)
        counts = jnp.where(lanes == block, count, counts)
    blocks = lanes[:1].astype(jnp.float32)
    least = jnp.min(counts, axis=0, keepdims=True)
    largest = jnp.max(counts, axis=0, keepdims=True)
    hot = jnp.min(jnp.where(least == most, blocks, float(n)), axis=1, keepdims=True)
    cold_most = jnp.max(jnp.where(blocks == hot, 0.0, largest), axis=1, keepdims=True)
    choice = jnp.full((1, 1), float(n * len(levels)), jnp.float32)
    for at in reversed(range(len(levels))):
        choice = jnp.where((cold_most <= levels[at]) & (hot < n), n * at + hot, choice)
    branch[0] = jnp.max(choice).astype(jnp.int32)


def gather(ids, picks, out_grads, n, dp, most, levels, rows_own):
    tok_count, width = out_grads.shape
    chunks = width // dp // LANES
    data = out_grads.reshape(tok_count // 8, 8, width // LANES, LANES).transpose(0, 2, 1, 3).reshape(-1, LANES)
    vmem, smem = pl.BlockSpec(memory_space=pltpu.VMEM), pl.BlockSpec(memory_space=pltpu.SMEM)
    return pl.pallas_call(
        functools.partial(gather_kernel, n, dp, most, levels, rows_own),
        out_shape=(
            jax.ShapeDtypeStruct((n * dp,) + ids.shape, ids.dtype),
            jax.ShapeDtypeStruct((dp, picks.shape[0], chunks, LANES), out_grads.dtype),
            jax.ShapeDtypeStruct((1,), jnp.int32),
        ),
        in_specs=[vmem, smem, pl.BlockSpec(memory_space=pltpu.HBM)],
        out_specs=(vmem, vmem, smem),
        scratch_shapes=[
            pltpu.VMEM(data.shape, data.dtype),
            pltpu.VMEM((tok_count * dp, chunks, LANES), data.dtype),
            pltpu.SemaphoreType.DMA,
            pltpu.SemaphoreType.DMA,
            pltpu.SemaphoreType.DMA((2,)),
        ],
        compiler_params=pltpu.CompilerParams(has_side_effects=True, vmem_limit_bytes=24 * 2**20),
        name="gather",
    )(ids, picks, data)


def flip(a, k, n):
    total, bit = 0, 1
    while bit < n:
        total = total + (((a // bit) % 2) + ((k // bit) % 2)) % 2 * bit
        bit *= 2
    return total


def exchange_kernel(n, dp, hot, most, few, picked_ref, arrived, sem_out, sem_in, own_sem):
    v, d = lax.axis_index("vocab"), lax.axis_index("dp")
    me = v * dp + d
    others = n * dp - 1

    def rows_of(block, column, count):
        source = picked_ref.at[column, pl.ds(block * most, count)]
        return source, arrived.at[pl.ds(me * most, count)]

    def send(i, _):
        k = i + 1
        block, column = flip(v, k // dp, n), (d + k % dp) % dp
        where = dict(device_id=(block, column), device_id_type=pl.DeviceIdType.MESH)

        @pl.when(block == hot)
        def _():
            pltpu.make_async_remote_copy(*rows_of(block, column, most), sem_out, sem_in, **where).start()

        @pl.when(block != hot)
        def _():
            pltpu.make_async_remote_copy(*rows_of(block, column, few), sem_out, sem_in, **where).start()

        return 0

    lax.fori_loop(0, others, send, 0)
    own = pltpu.make_async_copy(*rows_of(v, d, most), own_sem)
    own.start()
    own.wait()

    def drain(sem, count):
        rows = arrived.at[pl.ds(0, count)]
        pltpu.make_async_copy(rows, rows, sem).wait()

    @pl.when(v == hot)
    def _():
        drain(sem_out, (dp - 1) * most + (n - 1) * dp * few)
        drain(sem_in, others * most)

    @pl.when(v != hot)
    def _():
        drain(sem_out, dp * most + ((n - 1) * dp - 1) * few)
        drain(sem_in, others * few)


def exchange(n, dp, most, hot, few, picked):
    name = "exchange_all" if few == most else f"exchange_{hot}_{few}"
    return pl.pallas_call(
        functools.partial(exchange_kernel, n, dp, hot, most, few),
        out_shape=jax.ShapeDtypeStruct((n * dp * most,) + picked.shape[2:], picked.dtype),
        in_specs=[pl.BlockSpec(memory_space=pltpu.VMEM)],
        out_specs=pl.BlockSpec(memory_space=pl.ANY),
        scratch_shapes=[pltpu.SemaphoreType.DMA] * 3,
        compiler_params=pltpu.CompilerParams(has_side_effects=True, vmem_limit_bytes=24 * 2**20),
        name=name,
    )(picked)


def order_slots(ids_all, block, rows_own, capacity, tile):
    devices = ids_all.shape[0]
    mine = (ids_all // rows_own) == block
    positions = lax.iota(jnp.int32, ids_all.shape[1])
    before = mine[:, None, :] & (positions[None, None, :] < positions[None, :, None])
    rank = jnp.sum(before.astype(jnp.int32), axis=2)
    slot_ids = lax.iota(jnp.int32, capacity)
    hit = mine[:, None, :] & (rank[:, None, :] == slot_ids[None, :, None])
    local_row = ids_all - block * rows_own
    row_at = jnp.sum(jnp.where(hit, local_row[:, None, :] + 1, 0), axis=2) - 1
    row_at = row_at.reshape(-1)
    total = devices * capacity
    slots = lax.iota(jnp.int32, total)
    key = jnp.where(row_at >= 0, row_at, rows_own) * total + slots
    place = jnp.sum((key[None, :] < key[:, None]).astype(jnp.int32), axis=1)
    sorted_key = jnp.sum(jnp.where(place[None, :] == slots[:, None], key[None, :], 0), axis=1)
    sorted_row = sorted_key // total
    sorted_slot = sorted_key - sorted_row * total
    tiles = pl.cdiv(rows_own, tile)
    bounds = jnp.minimum(lax.iota(jnp.int32, tiles + 1) * tile, rows_own)
    row_key = key // total
    starts = jnp.sum((row_key[None, :] < bounds[:, None]).astype(jnp.int32), axis=1)
    return sorted_slot, sorted_row, starts


def table_kernel(tile, batch, slots_ref, rows_ref, starts_ref, data_ref, out_ref, data, acc, held, last_held, sems, data_sem):
    rows_own, width = out_ref.shape
    buffers = held.shape[0]
    full = rows_own // tile
    fetch = pltpu.make_async_copy(data_ref, data, data_sem)
    fetch.start()
    acc[...] = jnp.zeros_like(acc)
    fetch.wait()

    def fill(step, target):
        base = step * tile
        start, end = starts_ref[step], starts_ref[step + 1]
        batches = (end - start + batch - 1) // batch

        def row_at(at):
            return jnp.where(at < end, rows_ref[at] - base, tile)

        def add(index, carry):
            total, last = carry
            for at in range(batch):
                at += start + index * batch
                row = row_at(at)
                total = jnp.where(row == last, total, 0.0) + data[slots_ref[at]]
                acc[pl.ds(row, 1), :] = total.reshape(1, width)
                last = row
            return total, last

        lax.fori_loop(0, batches, add, (jnp.zeros(data.shape[1:], acc.dtype), jnp.int32(-1)))
        target[...] = acc[: target.shape[0], :].astype(target.dtype)

        @pl.loop(0, batches)
        def _(index):
            for at in range(batch):
                acc[pl.ds(row_at(at + start + index * batch), 1), :] = jnp.zeros((1, width), acc.dtype)

    def put(step, slot):
        place = out_ref.at[pl.ds(pl.multiple_of(step * tile, tile), tile)]
        return pltpu.make_async_copy(held.at[slot], place, sems.at[slot])

    @pl.loop(0, full)
    def _(step):
        slot = step % buffers

        @pl.when(step >= buffers)
        def _():
            put(step - buffers, slot).wait()

        fill(step, held.at[slot])
        put(step, slot).start()

    if rows_own % tile:
        fill(full, last_held)
        rest = pltpu.make_async_copy(last_held, out_ref.at[pl.ds(full * tile, rows_own % tile)], data_sem)
        rest.start()
        rest.wait()
    for step in range(max(full - buffers, 0), full):
        put(step, step % buffers).wait()


def build_table(data, slots, rows, starts, rows_own, tile, buffers, batch):
    _, chunks, _ = data.shape
    width = chunks * LANES
    slots, rows = (jnp.pad(part, (0, batch)) for part in (slots, rows))
    return pl.pallas_call(
        functools.partial(table_kernel, tile, batch),
        out_shape=jax.ShapeDtypeStruct((rows_own, width), jnp.bfloat16),
        in_specs=[pl.BlockSpec(memory_space=pltpu.SMEM)] * 3 + [pl.BlockSpec(memory_space=pl.ANY)],
        out_specs=pl.BlockSpec(memory_space=pl.ANY),
        scratch_shapes=[
            pltpu.VMEM(data.shape, data.dtype),
            pltpu.VMEM((tile + 8, width), jnp.float32),
            pltpu.VMEM((buffers, tile, width), jnp.bfloat16),
            pltpu.VMEM((rows_own % tile or 16, width), jnp.bfloat16),
            pltpu.SemaphoreType.DMA((buffers,)),
            pltpu.SemaphoreType.DMA,
        ],
        compiler_params=pltpu.CompilerParams(vmem_limit_bytes=40 * 2**20),
        name="table",
    )(slots, rows, starts, data)


def local(out_grads, token_ids):
    owners, dp = lax.axis_size("vocab"), lax.axis_size("dp")
    tok_count, width = out_grads.shape
    rows_own = VOCAB // owners
    most = 3 * tok_count // owners
    tile = 512
    mean = (tok_count - most) / (owners - 1)
    levels = [min(most, math.ceil(mean + spread * math.sqrt(mean))) for spread in (2.3, 3.6)]

    owner_of = token_ids // rows_own
    rank = ranks_in_block(owner_of[None])[0]
    target = owner_of * most + rank
    tokens = lax.iota(jnp.int32, tok_count)
    hit = target[None, :] == lax.iota(jnp.int32, owners * most)[:, None]
    picks = jnp.sum(jnp.where(hit, tokens[None, :], 0), axis=1)

    ids_all, picked, branch = gather(token_ids[None], picks, out_grads, owners, dp, most, levels, rows_own)
    slots, rows, starts = order_slots(ids_all[:, 0], lax.axis_index("vocab"), rows_own, most, tile)

    sends = [functools.partial(exchange, owners, dp, most, block, few) for few in levels for block in range(owners)]
    sends.append(functools.partial(exchange, owners, dp, most, 0, most))
    data = lax.switch(branch[0], sends, picked)
    return build_table(data, slots, rows, starts, rows_own, tile, 8, 8)


def solution(mesh):
    in_specs = (P(("vocab", "dp"), None), P(("vocab", "dp")))
    out_specs = P("vocab", "dp")
    return jax.shard_map(local, mesh=mesh, in_specs=in_specs, out_specs=out_specs, check_vma=False)
```

```python
import functools
import math

import jax
import jax.numpy as jnp
from jax import lax
from jax.experimental import pallas as pl
from jax.experimental.pallas import tpu as pltpu
from jax.sharding import PartitionSpec as P

VOCAB = 128256
LANES = 128


def ranks_in_block(owner_of):
    positions = lax.iota(jnp.int32, owner_of.shape[1])
    earlier = (owner_of[:, :, None] == owner_of[:, None, :]) & (positions[None, None, :] < positions[None, :, None])
    return jnp.sum(earlier.astype(jnp.int32), axis=2)


def gather_kernel(
    n, dp, most, early, levels, rows_own, tile, ids_ref, picks_ref, data_ref,
    ids_all, picked, arrived, branch, order_rows, order_slots, starts,
    data, rows, keys, columns, ids_out, ids_in, sem_out, sem_in, own_sem,
):
    v, d = lax.axis_index("vocab"), lax.axis_index("dp")
    me = v * dp + d
    devices = n * dp
    others = devices - 1
    chunks = rows.shape[1]
    fetch = pltpu.make_async_copy(data_ref, data, own_sem.at[0])
    fetch.start()
    own = pltpu.make_async_copy(ids_ref, ids_all.at[me], own_sem.at[1])
    own.start()

    def send(i, _):
        k = others - i
        where = dict(device_id=(flip(v, k // dp, n), (d + k % dp) % dp), device_id_type=pl.DeviceIdType.MESH)
        pltpu.make_async_remote_copy(ids_ref, ids_all.at[me], ids_out, ids_in, **where).start()
        return 0

    lax.fori_loop(0, others, send, 0)
    fetch.wait()

    @pl.loop(0, rows.shape[0] // (8 * dp))
    def _(group):
        for token in range(8):
            for column in range(dp):
                first = group * (8 * chunks * dp) + column * (8 * chunks) + token
                rows[group * (8 * dp) + token * dp + column] = data[pl.ds(first, chunks, stride=8), :]

    @pl.loop(0, picks_ref.shape[0] // 8)
    def _(group):
        for at in range(8):
            slot = group * 8 + at
            token = picks_ref[slot]
            for column in range(dp):
                picked[column, slot] = rows[token * dp + column]

    own.wait()

    def rows_of(block, column):
        return picked.at[column, pl.ds(block * most, early)], arrived.at[pl.ds(me * early, early)]

    def send_early(i, _):
        k = i + 1
        block, column = flip(v, k // dp, n), (d + k % dp) % dp
        where = dict(device_id=(block, column), device_id_type=pl.DeviceIdType.MESH)
        pltpu.make_async_remote_copy(*rows_of(block, column), sem_out, sem_in, **where).start()
        return 0

    lax.fori_loop(0, others, send_early, 0)
    keep = pltpu.make_async_copy(*rows_of(v, d), own_sem.at[0])
    keep.start()

    all_ids = ids_all.at[pl.ds(0, others)]
    for sem in (ids_out, ids_in):
        pltpu.make_async_copy(all_ids, all_ids, sem).wait()

    ids = ids_all[:, 0, :]
    lanes = lax.broadcasted_iota(jnp.int32, (devices, LANES), 1)
    counts = jnp.zeros((devices, LANES), jnp.float32)
    for block in range(n):
        inside = (ids >= block * rows_own) & (ids < (block + 1) * rows_own)
        count = jnp.sum(jnp.where(inside, 1.0, 0.0), axis=1, keepdims=True)
        counts = jnp.where(lanes == block, count, counts)
    blocks = lanes[:1].astype(jnp.float32)
    least = jnp.min(counts, axis=0, keepdims=True)
    largest = jnp.max(counts, axis=0, keepdims=True)
    hot = jnp.min(jnp.where(least == most, blocks, float(n)), axis=1, keepdims=True)
    cold_most = jnp.max(jnp.where(blocks == hot, 0.0, largest), axis=1, keepdims=True)
    choice = jnp.full((1, 1), float(n * len(levels)), jnp.float32)
    for at in reversed(range(len(levels))):
        choice = jnp.where((cold_most <= levels[at]) & (hot < n), n * at + hot, choice)
    branch[0] = jnp.max(choice).astype(jnp.int32)

    total = devices * most
    tokens = ids.shape[1]
    below = ids - v * rows_own
    mine = (below >= 0) & (below < rows_own)
    upper = lax.broadcasted_iota(jnp.int32, (tokens, tokens), 0) <= lax.broadcasted_iota(jnp.int32, (tokens, tokens), 1)
    ranks = jnp.dot(
        jnp.where(mine, 1.0, 0.0), jnp.where(upper, 1.0, 0.0), preferred_element_type=jnp.float32
    ).astype(jnp.int32)
    ranks = jnp.where(mine, ranks, 0)
    offset = below.astype(jnp.float32) - rows_own

    def collect(rank, found):
        row = jnp.sum(jnp.where(ranks == rank + 1, offset, 0.0), axis=1, keepdims=True) + rows_own
        columns[rank] = jnp.broadcast_to(row, (devices, LANES))
        return jnp.where(lanes == rank, row, found)

    found = jnp.full((devices, LANES), float(rows_own), jnp.float32)
    found = lax.fori_loop(0, most, collect, found, unroll=max(1, min(most, 256 // devices)))
    device = lax.broadcasted_iota(jnp.int32, (devices, LANES), 0)
    key = found.astype(jnp.int32) * total + device * most + lanes
    keys[...] = jnp.where(lanes < most, key, 2**30)

    bounds = jnp.minimum(lanes[:1] * tile, rows_own).astype(jnp.float32)
    order_rows[...] = jnp.zeros_like(order_rows)
    order_slots[...] = jnp.zeros_like(order_slots)

    def place(rank, ahead):
        row = columns[rank]
        key = row.astype(jnp.int32) * total + device * most + rank
        slot = jnp.where(rank < early, device * early, devices * early + device * (most - early) - early) + rank

        def count(source, smaller):
            return smaller + jnp.where(keys[pl.ds(source, 1), :] < key, 1.0, 0.0)

        smaller = lax.fori_loop(
            0, devices, count, jnp.zeros((devices, LANES), jnp.float32), unroll=max(1, 1024 // devices)
        )
        spot = jnp.sum(smaller, axis=1, keepdims=True).astype(jnp.int32)
        for at in range(pl.cdiv(total, LANES)):
            here = spot == lanes + at * LANES
            for order, value in ((order_rows, row), (order_slots, slot.astype(jnp.float32))):
                part = jnp.sum(jnp.where(here, value, 0.0), axis=0, keepdims=True)
                order[at : at + 1, :] += part.astype(jnp.int32)
        return ahead + jnp.where(row < bounds, 1.0, 0.0)

    ahead = jnp.zeros((devices, LANES), jnp.float32)
    ahead = lax.fori_loop(0, most, place, ahead, unroll=max(1, min(most, 128 // devices)))
    starts[...] = jnp.sum(ahead, axis=0, keepdims=True).astype(jnp.int32)

    keep.wait()
    early_rows = arrived.at[pl.ds(0, others * early)]
    for sem in (sem_out, sem_in):
        pltpu.make_async_copy(early_rows, early_rows, sem).wait()


def gather(ids, picks, out_grads, n, dp, most, early, levels, rows_own, tile):
    tok_count, width = out_grads.shape
    chunks = width // dp // LANES
    devices = n * dp
    data = out_grads.reshape(tok_count // 8, 8, width // LANES, LANES).transpose(0, 2, 1, 3).reshape(-1, LANES)
    order = jax.ShapeDtypeStruct((pl.cdiv(devices * most + 1, 8 * LANES) * 8, LANES), jnp.int32)
    vmem, smem = pl.BlockSpec(memory_space=pltpu.VMEM), pl.BlockSpec(memory_space=pltpu.SMEM)
    hbm = pl.BlockSpec(memory_space=pltpu.HBM)
    return pl.pallas_call(
        functools.partial(gather_kernel, n, dp, most, early, levels, rows_own, tile),
        out_shape=(
            jax.ShapeDtypeStruct((devices,) + ids.shape, ids.dtype),
            jax.ShapeDtypeStruct((dp, picks.shape[0], chunks, LANES), out_grads.dtype),
            jax.ShapeDtypeStruct((devices * early, chunks, LANES), out_grads.dtype),
            jax.ShapeDtypeStruct((1,), jnp.int32),
            order,
            order,
            jax.ShapeDtypeStruct((1, LANES), jnp.int32),
        ),
        in_specs=[vmem, smem, hbm],
        out_specs=(vmem, vmem, hbm, smem, vmem, vmem, vmem),
        scratch_shapes=[
            pltpu.VMEM(data.shape, data.dtype),
            pltpu.VMEM((tok_count * dp, chunks, LANES), data.dtype),
            pltpu.VMEM((devices, LANES), jnp.int32),
            pltpu.VMEM((most, devices, LANES), jnp.float32),
        ]
        + [pltpu.SemaphoreType.DMA] * 4
        + [pltpu.SemaphoreType.DMA((2,))],
        compiler_params=pltpu.CompilerParams(has_side_effects=True, vmem_limit_bytes=55 * 2**20),
        name="gather",
    )(ids, picks, data)


def flip(a, k, n):
    total, bit = 0, 1
    while bit < n:
        total = total + (((a // bit) % 2) + ((k // bit) % 2)) % 2 * bit
        bit *= 2
    return total


def exchange_kernel(n, dp, hot, most, few, early, picked_ref, arrived, sem_out, sem_in, own_sem):
    v, d = lax.axis_index("vocab"), lax.axis_index("dp")
    me = v * dp + d
    others = n * dp - 1

    def rows_of(block, column, count):
        source = picked_ref.at[column, pl.ds(block * most + early, count)]
        return source, arrived.at[pl.ds(me * (most - early), count)]

    def send(i, _):
        k = i + 1
        block, column = flip(v, k // dp, n), (d + k % dp) % dp
        where = dict(device_id=(block, column), device_id_type=pl.DeviceIdType.MESH)

        @pl.when(block == hot)
        def _():
            pltpu.make_async_remote_copy(*rows_of(block, column, most - early), sem_out, sem_in, **where).start()

        @pl.when(block != hot)
        def _():
            pltpu.make_async_remote_copy(*rows_of(block, column, few - early), sem_out, sem_in, **where).start()

        return 0

    lax.fori_loop(0, others, send, 0)
    own = pltpu.make_async_copy(*rows_of(v, d, most - early), own_sem)
    own.start()
    own.wait()

    def drain(sem, count):
        rows = arrived.at[pl.ds(0, count)]
        pltpu.make_async_copy(rows, rows, sem).wait()

    @pl.when(v == hot)
    def _():
        drain(sem_out, (dp - 1) * (most - early) + (n - 1) * dp * (few - early))
        drain(sem_in, others * (most - early))

    @pl.when(v != hot)
    def _():
        drain(sem_out, dp * (most - early) + ((n - 1) * dp - 1) * (few - early))
        drain(sem_in, others * (few - early))


def exchange(n, dp, most, early, hot, few, picked):
    name = "exchange_all" if few == most else f"exchange_{hot}_{few}"
    return pl.pallas_call(
        functools.partial(exchange_kernel, n, dp, hot, most, few, early),
        out_shape=jax.ShapeDtypeStruct((n * dp * (most - early),) + picked.shape[2:], picked.dtype),
        in_specs=[pl.BlockSpec(memory_space=pltpu.VMEM)],
        out_specs=pl.BlockSpec(memory_space=pl.ANY),
        scratch_shapes=[pltpu.SemaphoreType.DMA] * 3,
        compiler_params=pltpu.CompilerParams(has_side_effects=True, vmem_limit_bytes=24 * 2**20),
        name=name,
    )(picked)


def table_kernel(
    tile, batch, slots_ref, rows_ref, starts_ref, early_ref, data_ref, out_ref, data, acc, held, last_held, sems, data_sem
):
    rows_own, width = out_ref.shape
    buffers = held.shape[0]
    full = rows_own // tile
    early = early_ref.shape[0]
    fetches = [
        pltpu.make_async_copy(early_ref, data.at[pl.ds(0, early)], sems.at[0]),
        pltpu.make_async_copy(data_ref, data.at[pl.ds(early, data_ref.shape[0])], sems.at[1]),
    ]
    for fetch in fetches:
        fetch.start()
    acc[...] = jnp.zeros_like(acc)
    for fetch in fetches:
        fetch.wait()

    def fill(step, target):
        base = step * tile
        start, end = starts_ref[step], starts_ref[step + 1]
        batches = (end - start + batch - 1) // batch

        def row_at(at):
            return jnp.where(at < end, rows_ref[at] - base, tile)

        def add(index, carry):
            total, last = carry
            for at in range(batch):
                at += start + index * batch
                row = row_at(at)
                total = jnp.where(row == last, total, 0.0) + data[slots_ref[at]]
                acc[pl.ds(row, 1), :] = total.reshape(1, width)
                last = row
            return total, last

        lax.fori_loop(0, batches, add, (jnp.zeros(data.shape[1:], acc.dtype), jnp.int32(-1)))
        height = target.shape[0]
        dense = end - start > height // 12

        @pl.when(dense)
        def _():
            target[...] = acc[:height, :].astype(target.dtype)
            acc[:height, :] = jnp.zeros((height, width), acc.dtype)

        @pl.when(jnp.logical_not(dense))
        def _():
            target[...] = acc[:height, :].astype(target.dtype)

            @pl.loop(0, batches)
            def _(index):
                for at in range(batch):
                    acc[pl.ds(row_at(at + start + index * batch), 1), :] = jnp.zeros((1, width), acc.dtype)

    def put(step, slot):
        place = out_ref.at[pl.ds(pl.multiple_of(step * tile, tile), tile)]
        return pltpu.make_async_copy(held.at[slot], place, sems.at[slot])

    @pl.loop(0, full)
    def _(step):
        slot = step % buffers

        @pl.when(step >= buffers)
        def _():
            put(step - buffers, slot).wait()

        fill(step, held.at[slot])
        put(step, slot).start()

    if rows_own % tile:
        fill(full, last_held)
        rest = pltpu.make_async_copy(last_held, out_ref.at[pl.ds(full * tile, rows_own % tile)], data_sem)
        rest.start()
        rest.wait()
    for step in range(max(full - buffers, 0), full):
        put(step, step % buffers).wait()


def build_table(early, data, slots, rows, starts, rows_own, tile, buffers, batch):
    _, chunks, _ = data.shape
    width = chunks * LANES
    return pl.pallas_call(
        functools.partial(table_kernel, tile, batch),
        out_shape=jax.ShapeDtypeStruct((rows_own, width), jnp.bfloat16),
        in_specs=[pl.BlockSpec(memory_space=pltpu.SMEM)] * 3 + [pl.BlockSpec(memory_space=pltpu.HBM)] * 2,
        out_specs=pl.BlockSpec(memory_space=pl.ANY),
        scratch_shapes=[
            pltpu.VMEM((early.shape[0] + data.shape[0],) + data.shape[1:], data.dtype),
            pltpu.VMEM((tile + 8, width), jnp.float32),
            pltpu.VMEM((buffers, tile, width), jnp.bfloat16),
            pltpu.VMEM((rows_own % tile or 16, width), jnp.bfloat16),
            pltpu.SemaphoreType.DMA((buffers,)),
            pltpu.SemaphoreType.DMA,
        ],
        compiler_params=pltpu.CompilerParams(vmem_limit_bytes=40 * 2**20),
        name="table",
    )(slots.reshape(-1), rows.reshape(-1), starts.reshape(-1), early, data)


def local(out_grads, token_ids):
    owners, dp = lax.axis_size("vocab"), lax.axis_size("dp")
    tok_count, width = out_grads.shape
    rows_own = VOCAB // owners
    most = 3 * tok_count // owners
    early = max(1, most // 12)
    tile = 512
    mean = (tok_count - most) / (owners - 1)
    levels = [min(most, math.ceil(mean + spread * math.sqrt(mean))) for spread in (2.3, 3.6)]

    owner_of = token_ids // rows_own
    rank = ranks_in_block(owner_of[None])[0]
    target = owner_of * most + rank
    tokens = lax.iota(jnp.int32, tok_count)
    hit = target[None, :] == lax.iota(jnp.int32, owners * most)[:, None]
    picks = jnp.sum(jnp.where(hit, tokens[None, :], 0), axis=1)

    _, picked, first, branch, rows, slots, starts = gather(
        token_ids[None], picks, out_grads, owners, dp, most, early, levels, rows_own, tile
    )
    send = functools.partial(exchange, owners, dp, most, early)
    sends = [functools.partial(send, block, few) for few in levels for block in range(owners)]
    sends.append(functools.partial(send, 0, most))
    data = lax.switch(branch[0], sends, picked)
    return build_table(first, data, slots, rows, starts, rows_own, tile, 8, 8)


def solution(mesh):
    in_specs = (P(("vocab", "dp"), None), P(("vocab", "dp")))
    out_specs = P("vocab", "dp")
    return jax.shard_map(local, mesh=mesh, in_specs=in_specs, out_specs=out_specs, check_vma=False)
```

```python
import functools
import math

import jax
import jax.numpy as jnp
from jax import lax
from jax.experimental import pallas as pl
from jax.experimental.pallas import tpu as pltpu
from jax.sharding import PartitionSpec as P

VOCAB = 128256
LANES = 128


def ranks_in_block(owner_of):
    positions = lax.iota(jnp.int32, owner_of.shape[1])
    earlier = (owner_of[:, :, None] == owner_of[:, None, :]) & (positions[None, None, :] < positions[None, :, None])
    return jnp.sum(earlier.astype(jnp.int32), axis=2)


def gather_kernel(
    n, dp, most, early, levels, rows_own, tile, ids_ref, picks_ref, data_ref,
    ids_all, picked, arrived, branch, order_rows, order_slots, starts,
    data, rows, keys, columns, ids_out, ids_in, sem_out, sem_in, own_sem,
):
    v, d = lax.axis_index("vocab"), lax.axis_index("dp")
    me = v * dp + d
    devices = n * dp
    others = devices - 1
    chunks = rows.shape[1]
    fetch = pltpu.make_async_copy(data_ref, data, own_sem.at[0])
    fetch.start()
    own = pltpu.make_async_copy(ids_ref, ids_all.at[me], own_sem.at[1])
    own.start()

    def send(i, _):
        k = others - i
        where = dict(device_id=(flip(v, k // dp, n), (d + k % dp) % dp), device_id_type=pl.DeviceIdType.MESH)
        pltpu.make_async_remote_copy(ids_ref, ids_all.at[me], ids_out, ids_in, **where).start()
        return 0

    lax.fori_loop(0, others, send, 0)
    fetch.wait()

    @pl.loop(0, rows.shape[0] // (8 * dp))
    def _(group):
        for token in range(8):
            for column in range(dp):
                first = group * (8 * chunks * dp) + column * (8 * chunks) + token
                rows[group * (8 * dp) + token * dp + column] = data[pl.ds(first, chunks, stride=8), :]

    def pack(block, first, last):
        for rank in range(first, last):
            slot = block * most + rank
            token = picks_ref[slot]
            for column in range(dp):
                picked[column, slot] = rows[token * dp + column]

    pl.loop(0, n)(lambda block: pack(block, 0, early))
    pack(0, early, most)
    own.wait()

    def rows_of(block, column):
        return picked.at[column, pl.ds(block * most, early)], arrived.at[pl.ds(me * early, early)]

    def send_early(i, _):
        k = i + 1
        block, column = flip(v, k // dp, n), (d + k % dp) % dp
        where = dict(device_id=(block, column), device_id_type=pl.DeviceIdType.MESH)
        pltpu.make_async_remote_copy(*rows_of(block, column), sem_out, sem_in, **where).start()
        return 0

    lax.fori_loop(0, others, send_early, 0)
    keep = pltpu.make_async_copy(*rows_of(v, d), own_sem.at[0])
    keep.start()
    pl.loop(1, n)(lambda block: pack(block, early, most))

    all_ids = ids_all.at[pl.ds(0, others)]
    for sem in (ids_out, ids_in):
        pltpu.make_async_copy(all_ids, all_ids, sem).wait()

    ids = ids_all[:, 0, :]
    lanes = lax.broadcasted_iota(jnp.int32, (devices, LANES), 1)
    counts = jnp.zeros((devices, LANES), jnp.float32)
    for block in range(n):
        inside = (ids >= block * rows_own) & (ids < (block + 1) * rows_own)
        count = jnp.sum(jnp.where(inside, 1.0, 0.0), axis=1, keepdims=True)
        counts = jnp.where(lanes == block, count, counts)
    blocks = lanes[:1].astype(jnp.float32)
    least = jnp.min(counts, axis=0, keepdims=True)
    largest = jnp.max(counts, axis=0, keepdims=True)
    hot = jnp.min(jnp.where(least == most, blocks, float(n)), axis=1, keepdims=True)
    cold_most = jnp.max(jnp.where(blocks == hot, 0.0, largest), axis=1, keepdims=True)
    choice = jnp.full((1, 1), float(n * len(levels)), jnp.float32)
    for at in reversed(range(len(levels))):
        choice = jnp.where((cold_most <= levels[at]) & (hot < n), n * at + hot, choice)
    branch[0] = jnp.max(choice).astype(jnp.int32)

    total = devices * most
    tokens = ids.shape[1]
    below = ids - v * rows_own
    mine = (below >= 0) & (below < rows_own)
    upper = lax.broadcasted_iota(jnp.int32, (tokens, tokens), 0) <= lax.broadcasted_iota(jnp.int32, (tokens, tokens), 1)
    ranks = jnp.dot(
        jnp.where(mine, 1.0, 0.0), jnp.where(upper, 1.0, 0.0), preferred_element_type=jnp.float32
    ).astype(jnp.int32)
    ranks = jnp.where(mine, ranks, 0)
    offset = below.astype(jnp.float32) - rows_own

    def collect(rank, found):
        row = jnp.sum(jnp.where(ranks == rank + 1, offset, 0.0), axis=1, keepdims=True) + rows_own
        columns[rank] = jnp.broadcast_to(row, (devices, LANES))
        return jnp.where(lanes == rank, row, found)

    found = jnp.full((devices, LANES), float(rows_own), jnp.float32)
    found = lax.fori_loop(0, most, collect, found, unroll=max(1, min(most, 256 // devices)))
    device = lax.broadcasted_iota(jnp.int32, (devices, LANES), 0)
    key = found.astype(jnp.int32) * total + device * most + lanes
    keys[...] = jnp.where(lanes < most, key, 2**30)

    bounds = jnp.minimum(lanes[:1] * tile, rows_own).astype(jnp.float32)
    order_rows[...] = jnp.zeros_like(order_rows)
    order_slots[...] = jnp.zeros_like(order_slots)

    def place(rank, ahead):
        row = columns[rank]
        key = row.astype(jnp.int32) * total + device * most + rank
        slot = jnp.where(rank < early, device * early, devices * early + device * (most - early) - early) + rank

        def count(source, smaller):
            return smaller + jnp.where(keys[pl.ds(source, 1), :] < key, 1.0, 0.0)

        smaller = lax.fori_loop(
            0, devices, count, jnp.zeros((devices, LANES), jnp.float32), unroll=max(1, 1024 // devices)
        )
        spot = jnp.sum(smaller, axis=1, keepdims=True).astype(jnp.int32)
        for at in range(pl.cdiv(total, LANES)):
            here = spot == lanes + at * LANES
            for order, value in ((order_rows, row), (order_slots, slot.astype(jnp.float32))):
                part = jnp.sum(jnp.where(here, value, 0.0), axis=0, keepdims=True)
                order[at : at + 1, :] += part.astype(jnp.int32)
        return ahead + jnp.where(row < bounds, 1.0, 0.0)

    ahead = jnp.zeros((devices, LANES), jnp.float32)
    ahead = lax.fori_loop(0, most, place, ahead, unroll=max(1, min(most, 128 // devices)))
    starts[...] = jnp.sum(ahead, axis=0, keepdims=True).astype(jnp.int32)

    keep.wait()
    early_rows = arrived.at[pl.ds(0, others * early)]
    for sem in (sem_out, sem_in):
        pltpu.make_async_copy(early_rows, early_rows, sem).wait()


def gather(ids, picks, out_grads, n, dp, most, early, levels, rows_own, tile):
    tok_count, width = out_grads.shape
    chunks = width // dp // LANES
    devices = n * dp
    data = out_grads.reshape(tok_count // 8, 8, width // LANES, LANES).transpose(0, 2, 1, 3).reshape(-1, LANES)
    order = jax.ShapeDtypeStruct((pl.cdiv(devices * most + 1, 8 * LANES) * 8, LANES), jnp.int32)
    vmem, smem = pl.BlockSpec(memory_space=pltpu.VMEM), pl.BlockSpec(memory_space=pltpu.SMEM)
    hbm = pl.BlockSpec(memory_space=pltpu.HBM)
    return pl.pallas_call(
        functools.partial(gather_kernel, n, dp, most, early, levels, rows_own, tile),
        out_shape=(
            jax.ShapeDtypeStruct((devices,) + ids.shape, ids.dtype),
            jax.ShapeDtypeStruct((dp, picks.shape[0], chunks, LANES), out_grads.dtype),
            jax.ShapeDtypeStruct((devices * early, chunks, LANES), out_grads.dtype),
            jax.ShapeDtypeStruct((1,), jnp.int32),
            order,
            order,
            jax.ShapeDtypeStruct((1, LANES), jnp.int32),
        ),
        in_specs=[vmem, smem, hbm],
        out_specs=(vmem, vmem, hbm, smem, vmem, vmem, vmem),
        scratch_shapes=[
            pltpu.VMEM(data.shape, data.dtype),
            pltpu.VMEM((tok_count * dp, chunks, LANES), data.dtype),
            pltpu.VMEM((devices, LANES), jnp.int32),
            pltpu.VMEM((most, devices, LANES), jnp.float32),
        ]
        + [pltpu.SemaphoreType.DMA] * 4
        + [pltpu.SemaphoreType.DMA((2,))],
        compiler_params=pltpu.CompilerParams(has_side_effects=True, vmem_limit_bytes=55 * 2**20),
        name="gather",
    )(ids, picks, data)


def flip(a, k, n):
    total, bit = 0, 1
    while bit < n:
        total = total + (((a // bit) % 2) + ((k // bit) % 2)) % 2 * bit
        bit *= 2
    return total


def exchange_kernel(n, dp, hot, most, few, early, picked_ref, arrived, sem_out, sem_in, own_sem):
    v, d = lax.axis_index("vocab"), lax.axis_index("dp")
    me = v * dp + d
    others = n * dp - 1

    def rows_of(block, column, count):
        source = picked_ref.at[column, pl.ds(block * most + early, count)]
        return source, arrived.at[pl.ds(me * (most - early), count)]

    def send(i, _):
        k = i + 1
        block, column = flip(v, k // dp, n), (d + k % dp) % dp
        where = dict(device_id=(block, column), device_id_type=pl.DeviceIdType.MESH)

        @pl.when(block == hot)
        def _():
            pltpu.make_async_remote_copy(*rows_of(block, column, most - early), sem_out, sem_in, **where).start()

        @pl.when(block != hot)
        def _():
            pltpu.make_async_remote_copy(*rows_of(block, column, few - early), sem_out, sem_in, **where).start()

        return 0

    lax.fori_loop(0, others, send, 0)
    own = pltpu.make_async_copy(*rows_of(v, d, most - early), own_sem)
    own.start()
    own.wait()

    def drain(sem, count):
        rows = arrived.at[pl.ds(0, count)]
        pltpu.make_async_copy(rows, rows, sem).wait()

    @pl.when(v == hot)
    def _():
        drain(sem_out, (dp - 1) * (most - early) + (n - 1) * dp * (few - early))
        drain(sem_in, others * (most - early))

    @pl.when(v != hot)
    def _():
        drain(sem_out, dp * (most - early) + ((n - 1) * dp - 1) * (few - early))
        drain(sem_in, others * (few - early))


def exchange(n, dp, most, early, hot, few, picked):
    name = "exchange_all" if few == most else f"exchange_{hot}_{few}"
    return pl.pallas_call(
        functools.partial(exchange_kernel, n, dp, hot, most, few, early),
        out_shape=jax.ShapeDtypeStruct((n * dp * (most - early),) + picked.shape[2:], picked.dtype),
        in_specs=[pl.BlockSpec(memory_space=pltpu.VMEM)],
        out_specs=pl.BlockSpec(memory_space=pl.ANY),
        scratch_shapes=[pltpu.SemaphoreType.DMA] * 3,
        compiler_params=pltpu.CompilerParams(has_side_effects=True, vmem_limit_bytes=24 * 2**20),
        name=name,
    )(picked)


def table_kernel(
    tile, batch, slots_ref, rows_ref, starts_ref, early_ref, data_ref, out_ref, data, acc, held, last_held, sems, data_sem
):
    rows_own, width = out_ref.shape
    buffers = held.shape[0]
    full = rows_own // tile
    early = early_ref.shape[0]
    fetches = [
        pltpu.make_async_copy(early_ref, data.at[pl.ds(0, early)], sems.at[0]),
        pltpu.make_async_copy(data_ref, data.at[pl.ds(early, data_ref.shape[0])], sems.at[1]),
    ]
    for fetch in fetches:
        fetch.start()
    acc[...] = jnp.zeros_like(acc)
    for fetch in fetches:
        fetch.wait()

    def fill(step, target):
        base = step * tile
        start, end = starts_ref[step], starts_ref[step + 1]
        batches = (end - start + batch - 1) // batch

        def row_at(at):
            return jnp.where(at < end, rows_ref[at] - base, tile)

        def add(index, carry):
            total, last = carry
            for at in range(batch):
                at += start + index * batch
                row = row_at(at)
                total = jnp.where(row == last, total, 0.0) + data[slots_ref[at]]
                acc[pl.ds(row, 1), :] = total.reshape(1, width)
                last = row
            return total, last

        lax.fori_loop(0, batches, add, (jnp.zeros(data.shape[1:], acc.dtype), jnp.int32(-1)))
        height = target.shape[0]
        dense = end - start > height // 12

        @pl.when(dense)
        def _():
            target[...] = acc[:height, :].astype(target.dtype)
            acc[:height, :] = jnp.zeros((height, width), acc.dtype)

        @pl.when(jnp.logical_not(dense))
        def _():
            target[...] = acc[:height, :].astype(target.dtype)

            @pl.loop(0, batches)
            def _(index):
                for at in range(batch):
                    acc[pl.ds(row_at(at + start + index * batch), 1), :] = jnp.zeros((1, width), acc.dtype)

    def put(step, slot):
        place = out_ref.at[pl.ds(pl.multiple_of(step * tile, tile), tile)]
        return pltpu.make_async_copy(held.at[slot], place, sems.at[slot])

    @pl.loop(0, full)
    def _(step):
        slot = step % buffers

        @pl.when(step >= buffers)
        def _():
            put(step - buffers, slot).wait()

        fill(step, held.at[slot])
        put(step, slot).start()

    if rows_own % tile:
        fill(full, last_held)
        rest = pltpu.make_async_copy(last_held, out_ref.at[pl.ds(full * tile, rows_own % tile)], data_sem)
        rest.start()
        rest.wait()
    for step in range(max(full - buffers, 0), full):
        put(step, step % buffers).wait()


def build_table(early, data, slots, rows, starts, rows_own, tile, buffers, batch):
    _, chunks, _ = data.shape
    width = chunks * LANES
    return pl.pallas_call(
        functools.partial(table_kernel, tile, batch),
        out_shape=jax.ShapeDtypeStruct((rows_own, width), jnp.bfloat16),
        in_specs=[pl.BlockSpec(memory_space=pltpu.SMEM)] * 3 + [pl.BlockSpec(memory_space=pltpu.HBM)] * 2,
        out_specs=pl.BlockSpec(memory_space=pl.ANY),
        scratch_shapes=[
            pltpu.VMEM((early.shape[0] + data.shape[0],) + data.shape[1:], data.dtype),
            pltpu.VMEM((tile + 8, width), jnp.float32),
            pltpu.VMEM((buffers, tile, width), jnp.bfloat16),
            pltpu.VMEM((rows_own % tile or 16, width), jnp.bfloat16),
            pltpu.SemaphoreType.DMA((buffers,)),
            pltpu.SemaphoreType.DMA,
        ],
        compiler_params=pltpu.CompilerParams(vmem_limit_bytes=40 * 2**20),
        name="table",
    )(slots.reshape(-1), rows.reshape(-1), starts.reshape(-1), early, data)


def local(out_grads, token_ids):
    owners, dp = lax.axis_size("vocab"), lax.axis_size("dp")
    tok_count, width = out_grads.shape
    rows_own = VOCAB // owners
    most = 3 * tok_count // owners
    early = max(1, most // 12)
    tile = 1024
    mean = (tok_count - most) / (owners - 1)
    levels = [min(most, math.ceil(mean + spread * math.sqrt(mean))) for spread in (2.1, 2.7, 3.6)]

    owner_of = token_ids // rows_own
    rank = ranks_in_block(owner_of[None])[0]
    target = owner_of * most + rank
    tokens = lax.iota(jnp.int32, tok_count)
    hit = target[None, :] == lax.iota(jnp.int32, owners * most)[:, None]
    picks = jnp.sum(jnp.where(hit, tokens[None, :], 0), axis=1)

    _, picked, first, branch, rows, slots, starts = gather(
        token_ids[None], picks, out_grads, owners, dp, most, early, levels, rows_own, tile
    )
    send = functools.partial(exchange, owners, dp, most, early)
    sends = [functools.partial(send, block, few) for few in levels for block in range(owners)]
    sends.append(functools.partial(send, 0, most))
    data = lax.switch(branch[0], sends, picked)
    return build_table(first, data, slots, rows, starts, rows_own, tile, 4, 8)


def solution(mesh):
    in_specs = (P(("vocab", "dp"), None), P(("vocab", "dp")))
    out_specs = P("vocab", "dp")
    return jax.shard_map(local, mesh=mesh, in_specs=in_specs, out_specs=out_specs, check_vma=False)
```
